32 devices in a mesh: dp: 4 (over y, z), tp: 8 (over x, core).
Axes of the slice: x: 4, y: 2, z: 2, core: 2. Of those that a mesh axis runs over, the one named last changes fastest.
The devices are a block of a 4x4x8 slice.
Arguments:
- hidden: bfloat16 [4, 3072, 1536], P('dp', 'tp'), parts along dimension 0
- targets: int32 [4, 3072], P('dp', 'tp'), parts along dimension 0
- norm_gain: bfloat16 [1536], replicated
- head_w: bfloat16 [151936, 1536], P('tp')
- temperature: float32 [], replicated
Outputs:
- output 1: float32 [4, 3072], P('dp', 'tp'), parts along dimension 0
- output 2: float32 [4, 3072], P('dp', 'tp'), parts along dimension 0
There are 4 independent parts. The reference program is written for one: setup_inputs(seed, part) draws one part's arguments, and reference() takes and returns one part's arrays. A program takes and returns all parts, laid end to end along the dimension named above; an argument that names none is the same for every part.
All inputs are finite; a program needn't handle non-finite values.
Results may differ from the reference program's by a relative error of at most 0.001.
Values are sent between devices in bfloat16 or wider.
A program may use at most 768 MiB of HBM per device.

```python
import jax
import jax.numpy as jnp
from jax import lax

ROW_COUNT = 1
SEQ_LEN = 3072
BLOCK_TOKENS = 384
MODEL_DIM = 1536
VOCAB_SIZE = 151936
NORM_EPS = 1e-6
PEAK_SCALE = 10.0


def setup_inputs(seed: int = 0, part: int = 0) -> dict:
    base_key = jax.random.key(seed)
    part_key = jax.random.fold_in(base_key, part)
    key_head, key_gain, key_temp = jax.random.split(base_key, 3)
    key_noise, key_peak, key_coin, key_spread = jax.random.split(part_key, 4)
    head_wide = jax.random.normal(key_head, (VOCAB_SIZE, MODEL_DIM), jnp.float32) * MODEL_DIM ** -0.5
    gain_wide = 1.0 + 0.3 * jax.random.normal(key_gain, (MODEL_DIM,), jnp.float32)
    temperature = jax.random.uniform(key_temp, (), jnp.float32, 0.6, 0.9)
    peak_ids = jax.random.randint(key_peak, (ROW_COUNT, SEQ_LEN), 0, VOCAB_SIZE)
    noise_part = jax.random.normal(key_noise, (ROW_COUNT, SEQ_LEN, MODEL_DIM), jnp.float32)
    hidden = noise_part + PEAK_SCALE * head_wide[peak_ids]
    coin_flip = jax.random.randint(key_coin, (ROW_COUNT, SEQ_LEN), 0, 2)
    spread_ids = jax.random.randint(key_spread, (ROW_COUNT, SEQ_LEN), 0, VOCAB_SIZE)
    targets = jnp.where(coin_flip == 1, peak_ids, spread_ids).astype(jnp.int32)
    return dict(hidden=hidden.astype(jnp.bfloat16), targets=targets, norm_gain=gain_wide.astype(jnp.bfloat16), head_w=head_wide.astype(jnp.bfloat16), temperature=temperature)


def reference(hidden, targets, norm_gain, head_w, temperature):
    h_wide = hidden.astype(jnp.float32)
    inv_rms = lax.rsqrt(jnp.mean(h_wide * h_wide, axis=-1, keepdims=True) + NORM_EPS)
    normed = (norm_gain.astype(jnp.float32) * h_wide * inv_rms).astype(jnp.bfloat16)
    block_count = ROW_COUNT * SEQ_LEN // BLOCK_TOKENS
    row_blocks = normed.reshape(block_count, BLOCK_TOKENS, MODEL_DIM)
    target_blocks = targets.reshape(block_count, BLOCK_TOKENS)

    def block_stats(pair):
        rows_blk, target_blk = pair
        logits = jnp.dot(rows_blk, head_w.T, preferred_element_type=jnp.float32) / temperature
        top_val = jnp.max(logits, axis=-1, keepdims=True)
        exp_shift = jnp.exp(logits - top_val)
        sum_exp = jnp.sum(exp_shift, axis=-1)
        weighted = jnp.sum(exp_shift * logits, axis=-1)
        log_norm = top_val[:, 0] + jnp.log(sum_exp)
        target_logit = jnp.take_along_axis(logits, target_blk[:, None], axis=-1)[:, 0]
        return target_logit - log_norm, log_norm - weighted / sum_exp

    log_prob, entropy = lax.map(block_stats, (row_blocks, target_blocks))
    return log_prob.reshape(ROW_COUNT, SEQ_LEN), entropy.reshape(ROW_COUNT, SEQ_LEN)
```

```python
import functools

import jax
import jax.numpy as jnp
from jax import lax
from jax.experimental import pallas as pl
from jax.experimental.pallas import tpu as pltpu
from jax.sharding import PartitionSpec as P

NORM_EPS = 1e-6
LOG2E = 1.4426950408889634
LOWEST = -3.4028234e38
SIDE = 256
M_ROWS = 432
PIECE = 48
SUBS = 2
RELAY_TRIP = 7
MESH = pl.DeviceIdType.MESH


def _kernel(dims, h_ref, tgt_ref, gain_ref, tau_ref, w_ref, lp_ref, ent_ref,
            h_buf, x_all, tgt_all, w_buf, z_buf, st_m, st_s, st_w, st_t, c_buf, stage, inbox,
            h_sem, w_sem, x_send, x_recv, t_send, t_recv, s_send, s_recv):
    n_tp, tok, depth, vocab = dims
    chips = n_tp // 2
    pair = 2 * tok
    blocks = pair // SIDE
    n_k = depth // SIDE
    sub_rows = 2 * M_ROWS
    tile_rows = SUBS * sub_rows
    n_tiles = -(-vocab // tile_rows)
    overlap = n_tiles * tile_rows - vocab
    units = SUBS * blocks
    n_stats = chips * blocks
    me = lax.axis_index('tp')
    x_pos, core = lax.div(me, 2), lax.rem(me, 2)

    def device(hops, other):
        return {'tp': lax.rem(x_pos + hops, chips) * 2 + (1 - core if other else core)}

    hops_of = {0: 0, 1: chips - 1, 2: 1, 3: 2}
    seen_as = {0: 0, 1: 2, 2: 1, 3: 3}
    peers = [(g, o) for g in range(chips) for o in (0, 1) if (g, o) != (0, 0)]

    def row_start(j):
        return pl.multiple_of(jnp.minimum(j * tile_rows, vocab - tile_rows), 16)

    def w_copy(q, s):
        j = lax.rem(q, n_tiles)
        return pltpu.make_async_copy(
            w_ref.at[pl.ds(pl.multiple_of(row_start(j) + s * sub_rows, 16), sub_rows)],
            w_buf.at[lax.rem(q, 2), pl.ds(s * sub_rows, sub_rows)],
            w_sem.at[lax.rem(q, 2), s],
        )

    h_copy = pltpu.make_async_copy(h_ref, h_buf, h_sem)
    h_copy.start()
    for s in range(SUBS):
        w_copy(0, s).start()
    barrier = pltpu.get_barrier_semaphore()
    for g, o in peers:
        pl.semaphore_signal(barrier, inc=1, device_id=device(hops_of[g], o), device_id_type=MESH)

    c_buf[...] = LOG2E / jnp.full(c_buf.shape, tau_ref[0, 0], jnp.float32)
    st_m[...] = jnp.full(st_m.shape, LOWEST, jnp.float32)
    for st in (st_s, st_w, st_t):
        st[...] = jnp.zeros(st.shape, jnp.float32)

    own_rows = pl.ds(pl.multiple_of(core * tok, 16), tok)
    own_lanes = pl.ds(pl.multiple_of(core * tok, 128), tok)
    h_copy.wait()

    norm_rows = 64

    @pl.loop(0, tok // norm_rows)
    def _(r):
        h = h_buf[pl.ds(pl.multiple_of(r * norm_rows, 16), norm_rows), :].astype(jnp.float32)
        inv = lax.rsqrt(jnp.mean(h * h, axis=-1, keepdims=True) + NORM_EPS)
        x = (gain_ref[...].astype(jnp.float32) * h * inv).astype(jnp.bfloat16)
        x_all[0, pl.ds(pl.multiple_of(core * tok + r * norm_rows, 16), norm_rows), :] = x

    pl.semaphore_wait(barrier, len(peers))

    def x_copy(src_g, dst_g, hops, other, send):
        return pltpu.make_async_remote_copy(
            src_ref=x_all.at[src_g, own_rows],
            dst_ref=x_all.at[dst_g, own_rows],
            send_sem=x_send.at[send],
            recv_sem=x_recv.at[dst_g * 2 + other],
            device_id=device(hops, other),
            device_id_type=MESH,
        )

    def x_arrival(g, other):
        rows = pl.ds(pl.multiple_of((1 - core if other else core) * tok, 16), tok)
        return pltpu.make_async_remote_copy(
            src_ref=x_all.at[g, rows],
            dst_ref=x_all.at[g, rows],
            send_sem=x_send.at[0],
            recv_sem=x_recv.at[g * 2 + other],
            device_id=device(0, 1),
            device_id_type=MESH,
        )

    def t_copy(g, o):
        n = g * 2 + o
        return pltpu.make_async_remote_copy(
            src_ref=tgt_ref,
            dst_ref=tgt_all.at[seen_as[g], :, own_lanes],
            send_sem=t_send.at[n],
            recv_sem=t_recv.at[seen_as[g] * 2 + o],
            device_id=device(hops_of[g], o),
            device_id_type=MESH,
        )

    own_copies = [x_copy(0, 1, 1, 0, 1), x_copy(0, 2, chips - 1, 0, 2), x_copy(0, 0, 0, 1, 0)]
    for copy in own_copies:
        copy.start()
    for g, o in peers:
        t_copy(g, o).start()
    tgt_all[0, :, own_lanes] = tgt_ref[...]

    far = x_copy(jnp.where(core == 0, 1, 2), 3, jnp.where(core == 0, 1, chips - 1), 0, 3)
    relays = [x_copy(1, 1, 0, 1, 4), x_copy(2, 2, 0, 1, 5), x_copy(3, 3, 0, 1, 6)]

    def t_wait(g, o):
        n = seen_as[g] * 2 + o
        pltpu.make_async_remote_copy(
            src_ref=tgt_ref,
            dst_ref=tgt_all.at[g, :, pl.ds(pl.multiple_of((1 - core if o else core) * tok, 128), tok)],
            send_sem=t_send.at[n],
            recv_sem=t_recv.at[g * 2 + o],
            device_id=device(0, 1),
            device_id_type=MESH,
        ).wait_recv()

    for g, o in peers:
        t_wait(g, o)
    x_arrival(0, 1).wait_recv()

    sublane = lax.broadcasted_iota(jnp.int32, (8, SIDE), 0)

    def place(t):
        first = t < n_tiles
        u = jnp.maximum(t - n_tiles, 0)
        j = jnp.where(first, t, lax.div(u, chips - 1))
        g = jnp.where(first, 0, 1 + lax.rem(u, chips - 1))
        q = jnp.where(first, t, n_tiles + lax.div(u, chips - 1))
        fresh = jnp.logical_or(first, lax.rem(u, chips - 1) == 0)
        return j, g, q, fresh

    def drain(accs, stat, base, bias, target):
        m_old = st_m[stat]
        top = m_old
        z = z_buf[accs]
        if bias is not None:
            head = z[:overlap].reshape(overlap // 8, 8, SIDE) + bias
            top = jnp.maximum(top, jnp.max(head, axis=0))
            z = z[overlap:]
        top = jnp.maximum(top, jnp.max(z.reshape(-1, 8, SIDE), axis=0))
        c = c_buf[...]
        alpha = jnp.exp2((m_old - top) * c)
        st_m[stat] = top
        state = [st_s[stat] * alpha, st_w[stat] * alpha, st_t[stat]]
        where = target - sublane - base
        for r in range(0, sub_rows, PIECE):
            z = z_buf[accs, pl.ds(r, PIECE), :].reshape(PIECE // 8, 8, SIDE)
            zb = z
            if bias is not None and r == 0:
                zb = jnp.concatenate([z[:overlap // 8] + bias, z[overlap // 8:]], axis=0)
            p = jnp.exp2((zb - top) * c)
            state[0] = state[0] + jnp.sum(p, axis=0)
            state[1] = state[1] + jnp.sum(p * z, axis=0)
            for i in range(PIECE // 8):
                state[2] = jnp.where(where == r + 8 * i, z[i], state[2])
        st_s[stat], st_w[stat], st_t[stat] = state

    def body():
        z_buf[1] = jnp.zeros(z_buf.shape[1:], jnp.float32)

        def trip(t, carry):
            j, g, q, fresh = place(t)
            slot = lax.rem(q, 2)

            @pl.when(fresh)
            def _():
                @pl.when(q + 1 < 2 * n_tiles)
                def _():
                    for s in range(SUBS):
                        w_copy(q + 1, s).start()
                for s in range(SUBS):
                    w_copy(q, s).wait()

            @pl.when(t == RELAY_TRIP)
            def _():
                x_arrival(1, 0).wait_recv()
                x_arrival(2, 0).wait_recv()
                far.start()
                relays[0].start()
                relays[1].start()

            @pl.when(t == n_tiles)
            def _():
                x_arrival(1, 1).wait_recv()
                x_arrival(2, 1).wait_recv()

            @pl.when(t == n_tiles + 1)
            def _():
                x_arrival(3, 0).wait_recv()
                relays[2].start()

            @pl.when(t == n_tiles + 2)
            def _():
                x_arrival(3, 1).wait_recv()

            shard_base = me * vocab + row_start(j)
            bias = jnp.where(j == n_tiles - 1, LOWEST, 0.0).astype(jnp.float32)
            pj, pg, _, _ = place(jnp.maximum(t - 1, 0))
            for i in range(units):
                s, b = divmod(i, blocks)
                z_buf[i % 2] = lax.dot_general(
                    w_buf[slot, pl.ds(s * sub_rows, sub_rows), :], x_all[g, pl.ds(b * SIDE, SIDE), :],
                    (((1,), (1,)), ((), ())), preferred_element_type=jnp.float32)
                if i == 0:
                    stat = jnp.where(t == 0, n_stats, pg * blocks + blocks - 1)
                    base = me * vocab + row_start(pj) + (SUBS - 1) * sub_rows
                    target = tgt_all[pg, :, (blocks - 1) * SIDE:blocks * SIDE]
                    drain(1, stat, base, None, target)
                else:
                    ps, pb = divmod(i - 1, blocks)
                    target = tgt_all[g, :, pb * SIDE:(pb + 1) * SIDE]
                    drain((i - 1) % 2, g * blocks + pb, shard_base + ps * sub_rows,
                          bias if ps == 0 else None, target)
            return carry

        trips = n_tiles * chips
        lax.fori_loop(0, trips, trip, 0)
        pj, pg, _, _ = place(trips - 1)
        drain(1, pg * blocks + blocks - 1, me * vocab + row_start(pj) + (SUBS - 1) * sub_rows, None,
              tgt_all[pg, :, (blocks - 1) * SIDE:blocks * SIDE])

    body()

    c1 = c_buf[0:1, :]
    for g in range(chips):
        for b in range(blocks):
            n, lanes = g * blocks + b, slice(b * SIDE, (b + 1) * SIDE)
            m = st_m[n]
            top = jnp.max(m, axis=0, keepdims=True)
            f = jnp.exp2((m - top) * c1)
            stage[g, 0:1, lanes] = top
            stage[g, 1:2, lanes] = jnp.sum(st_s[n] * f, axis=0, keepdims=True)
            stage[g, 2:3, lanes] = jnp.sum(st_w[n] * f, axis=0, keepdims=True)
            stage[g, 3:4, lanes] = jnp.sum(st_t[n], axis=0, keepdims=True)
            stage[g, 4:8, lanes] = jnp.zeros((4, SIDE), jnp.float32)

    def s_copy(g, o):
        n = g * 2 + o
        lanes = pl.ds(pl.multiple_of((1 - core if o else core) * tok, 128), tok)
        return pltpu.make_async_remote_copy(
            src_ref=stage.at[g, :, lanes],
            dst_ref=inbox.at[seen_as[g] * 2 + o],
            send_sem=s_send.at[n],
            recv_sem=s_recv.at[seen_as[g] * 2 + o],
            device_id=device(hops_of[g], o),
            device_id_type=MESH,
        )

    s_copies = [s_copy(g, o) for g, o in peers]
    for copy in s_copies:
        copy.start()
    inbox[0] = stage[0, :, own_lanes]
    for copy in s_copies:
        copy.wait()
    got = [inbox[n] for n in range(n_tp)]
    top = functools.reduce(jnp.maximum, [x[0:1] for x in got])
    c2 = jnp.concatenate([c1, c1], axis=1)[:, :tok]
    scales = [jnp.exp2((x[0:1] - top) * c2) for x in got]
    total = functools.reduce(jnp.add, [x[1:2] * f for x, f in zip(got, scales)])
    weighted = functools.reduce(jnp.add, [x[2:3] * f for x, f in zip(got, scales)])
    target = functools.reduce(jnp.add, [x[3:4] for x in got])
    tau = jnp.full(top.shape, tau_ref[0, 0], jnp.float32)
    log_norm = top / tau + jnp.log(total)
    lp_ref[...] = target / tau - log_norm
    ent_ref[...] = log_norm - (weighted / total) / tau

    for copy in own_copies + [far] + relays:
        copy.wait_send()
    for g, o in peers:
        t_copy(g, o).wait_send()


def solution(mesh):
    n_tp = mesh.shape['tp']

    def device_body(h_loc, target_loc, norm_gain, w_loc, tau):
        _, tok, depth = h_loc.shape
        vocab = w_loc.shape[0]
        pair, chips = 2 * tok, n_tp // 2
        blocks = pair // SIDE
        n_stats = chips * blocks
        any_space = pl.BlockSpec(memory_space=pl.ANY)
        vmem = pl.BlockSpec(memory_space=pltpu.VMEM)
        stat = pltpu.VMEM((n_stats + 1, 8, SIDE), jnp.float32)
        dma = pltpu.SemaphoreType.DMA
        return pl.pallas_call(
            functools.partial(_kernel, (n_tp, tok, depth, vocab)),
            out_shape=(jax.ShapeDtypeStruct((1, tok), jnp.float32),) * 2,
            in_specs=[any_space, vmem, vmem, pl.BlockSpec(memory_space=pltpu.SMEM), any_space],
            out_specs=(vmem, vmem),
            scratch_shapes=[
                pltpu.VMEM((tok, depth), jnp.bfloat16),
                pltpu.VMEM((chips, pair, depth), jnp.bfloat16),
                pltpu.VMEM((chips, 1, pair), jnp.int32),
                pltpu.VMEM((2, SUBS * 2 * M_ROWS, depth), jnp.bfloat16),
                pltpu.VMEM((2, 2 * M_ROWS, SIDE), jnp.float32),
                stat, stat, stat, stat,
                pltpu.VMEM((8, SIDE), jnp.float32),
                pltpu.VMEM((chips, 8, pair), jnp.float32),
                pltpu.VMEM((n_tp, 8, tok), jnp.float32),
                dma(()), dma((2, SUBS)), dma((7,)), dma((n_tp,)), dma((n_tp,)), dma((n_tp,)), dma((n_tp,)), dma((n_tp,)),
            ],
            compiler_params=pltpu.CompilerParams(
                collective_id=0, has_side_effects=True, vmem_limit_bytes=60 * 1024 * 1024),
        )(h_loc[0], target_loc, norm_gain.reshape(1, depth), tau.reshape(1, 1), w_loc)

    return jax.shard_map(
        device_body,
        mesh=mesh,
        in_specs=(P('dp', 'tp', None), P('dp', 'tp'), P(), P('tp', None), P()),
        out_specs=(P('dp', 'tp'), P('dp', 'tp')),
        check_vma=False,
    )
```

```python
import functools

import jax
import jax.numpy as jnp
from jax import lax
from jax.experimental import pallas as pl
from jax.experimental.pallas import tpu as pltpu
from jax.sharding import PartitionSpec as P

NORM_EPS = 1e-6
LOG2E = 1.4426950408889634
LOWEST = -3.4028234e38
SIDE = 256
UNIT_ROWS = 864
SUBS = 2
PIECE = 48
NORM_ROWS = 64
W_SLOTS = 4
MESH = pl.DeviceIdType.MESH

OWNER = {(0, 1): (0, 1), (1, 0): (-1, 0), (1, 1): (1, 0), (2, 0): (-1, 1), (2, 1): (1, 1), (3, 0): (2, 0), (3, 1): (2, 1)}
SEEN_AS = {(0, 1): (0, 1), (1, 0): (1, 1), (1, 1): (1, 0), (2, 0): (2, 1), (2, 1): (2, 0), (3, 0): (3, 0), (3, 1): (3, 1)}


def _kernel(dims, h_ref, tgt_ref, gain_ref, tau_ref, w_ref, out_ref,
            h_buf, x_all, tgt_all, w_buf, z_buf, z_top, st_m, st_s, st_w, st_t, c_buf, stage, inbox,
            h_sem, w_sem, x_send, x_recv, t_send, t_recv, s_send, s_recv):
    n_tp, tok, depth, vocab = dims
    chips = n_tp // 2
    pair = 2 * tok
    blocks = pair // SIDE
    tile_rows = SUBS * UNIT_ROWS
    n_tiles = -(-vocab // tile_rows)
    overlap = n_tiles * tile_rows - vocab
    half_units = SUBS * blocks
    n_stats = chips * blocks
    me = lax.axis_index('tp')
    x_pos, core = lax.div(me, 2), lax.rem(me, 2)

    def device(hops, other):
        return {'tp': lax.rem(x_pos + hops + chips, chips) * 2 + (1 - core if other else core)}

    def row_start(j):
        return pl.multiple_of(jnp.minimum(j * tile_rows, vocab - tile_rows), 16)

    def w_copy(q, s):
        slot = lax.rem(q, W_SLOTS)
        return pltpu.make_async_copy(
            w_ref.at[pl.ds(pl.multiple_of(row_start(lax.rem(q, n_tiles)) + s * UNIT_ROWS, 16), UNIT_ROWS)],
            w_buf.at[slot, pl.ds(s * UNIT_ROWS, UNIT_ROWS)],
            w_sem.at[slot, s],
        )

    def w_start(q):
        for s in range(SUBS):
            w_copy(q, s).start()

    def w_wait(q):
        for s in range(SUBS):
            w_copy(q, s).wait()

    h_copy = pltpu.make_async_copy(h_ref, h_buf, h_sem)
    h_copy.start()
    w_start(0)
    w_start(1)
    barrier = pltpu.get_barrier_semaphore()
    for hops, other in OWNER.values():
        pl.semaphore_signal(barrier, inc=1, device_id=device(hops, other), device_id_type=MESH)

    c_buf[...] = LOG2E / jnp.full(c_buf.shape, tau_ref[0, 0], jnp.float32)
    st_m[...] = jnp.full(st_m.shape, LOWEST, jnp.float32)
    for st in (st_s, st_w, st_t):
        st[...] = jnp.zeros(st.shape, jnp.float32)
    z_top[...] = jnp.zeros(z_top.shape, jnp.float32)
    for n in (2, 3):
        z_buf[n] = jnp.zeros(z_buf.shape[1:], jnp.float32)

    h_copy.wait()
    gain = gain_ref[...].astype(jnp.float32).reshape(1, depth)

    @pl.loop(0, tok // NORM_ROWS)
    def _(r):
        rows = pl.ds(pl.multiple_of(r * NORM_ROWS, 16), NORM_ROWS)
        h = h_buf[rows, :].astype(jnp.float32)
        inv = lax.rsqrt(jnp.mean(h * h, axis=-1, keepdims=True) + NORM_EPS)
        x_all[0, rows, :] = (gain * h * inv).astype(jnp.bfloat16)

    pl.semaphore_wait(barrier, len(OWNER))

    def chunk(p, f):
        return x_all.at[p, pl.ds(f * tok if isinstance(f, int) else pl.multiple_of(f * tok, 16), tok)]

    def x_copy(src, dst, hops, other, send):
        return pltpu.make_async_remote_copy(
            src_ref=chunk(*src),
            dst_ref=chunk(*dst),
            send_sem=x_send.at[send],
            recv_sem=x_recv.at[dst[0] * 2 + dst[1]],
            device_id=device(hops, other),
            device_id_type=MESH,
        )

    def x_wait(p, f):
        x_copy((p, f), (p, f), 0, 1, 0).wait_recv()

    def t_copy(where):
        p, f = SEEN_AS[where]
        return pltpu.make_async_remote_copy(
            src_ref=tgt_ref,
            dst_ref=tgt_all.at[p, :, pl.ds(f * tok, tok)],
            send_sem=t_send.at[where[0] * 2 + where[1]],
            recv_sem=t_recv.at[p * 2 + f],
            device_id=device(*OWNER[where]),
            device_id_type=MESH,
        )

    t_copies = {where: t_copy(where) for where in OWNER}
    t_waits = {SEEN_AS[where]: copy for where, copy in t_copies.items()}
    for copy in t_copies.values():
        copy.start()
    own_copies = [x_copy((0, 0), (0, 1), 0, 1, 0), x_copy((0, 0), (1, 0), 1, 0, 1), x_copy((0, 0), (1, 1), -1, 0, 2)]
    for copy in own_copies:
        copy.start()
    tgt_all[0, :, 0:tok] = tgt_ref[...]

    far = x_copy((1, jnp.where(core == 0, 0, 1)), (3, 0), jnp.where(core == 0, 1, -1), 0, 3)
    to_other = [x_copy((1, 0), (2, 0), 0, 1, 4), x_copy((1, 1), (2, 1), 0, 1, 5), x_copy((3, 0), (3, 1), 0, 1, 6)]

    t_waits[(0, 1)].wait_recv()
    x_wait(0, 1)

    sublane = lax.broadcasted_iota(jnp.int32, (8, SIDE), 0)

    def place(h):
        late = h >= 3 * n_tiles
        first = h < n_tiles
        u = jnp.maximum(h - n_tiles, 0)
        j = jnp.where(first, h, jnp.where(late, h - 3 * n_tiles, lax.div(u, 2)))
        g = jnp.where(first, 0, jnp.where(late, 3, 1 + lax.rem(u, 2)))
        q = jnp.where(first, h, jnp.where(late, h - n_tiles, n_tiles + lax.div(u, 2)))
        return j, g, q

    def drain(slot, stat, base, bias, target):
        m_old = st_m[stat]
        top = jnp.maximum(m_old, z_top[slot])
        if bias is not None:
            head = z_buf[slot, 0:overlap, :].reshape(overlap // 8, 8, SIDE) + bias
            top = jnp.maximum(top, jnp.max(head, axis=0))
        c = c_buf[...]
        alpha = jnp.exp2((m_old - top) * c)
        st_m[stat] = top
        total, weighted, hit = st_s[stat] * alpha, st_w[stat] * alpha, st_t[stat]
        row = target - sublane - base
        for r in range(0, UNIT_ROWS, PIECE):
            z = z_buf[slot, pl.ds(r, PIECE), :].reshape(PIECE // 8, 8, SIDE)
            zb = z
            if bias is not None and r == 0:
                zb = jnp.concatenate([z[:overlap // 8] + bias, z[overlap // 8:]], axis=0)
            p = jnp.exp2((zb - top) * c)
            total = total + jnp.sum(p, axis=0)
            weighted = weighted + jnp.sum(p * z, axis=0)
            for i in range(PIECE // 8):
                hit = jnp.where(row == r + 8 * i, z[i], hit)
        st_s[stat], st_w[stat], st_t[stat] = total, weighted, hit

    def high(t):
        return place(2 * t + 1)[2]

    trips = n_tiles * chips // 2

    def drain_last(t, i, valid):
        j, g, _ = place(2 * t + 1)
        s, b = divmod(i, blocks)
        stat = g * blocks + b if valid is None else jnp.where(valid, g * blocks + b, n_stats)
        drain(2 + (i - (half_units - 2)), stat, me * vocab + row_start(j) + s * UNIT_ROWS, None,
              tgt_all[g, :, b * SIDE:(b + 1) * SIDE])

    def trip(t, carry):
        now, before, after = high(t), high(t - 1), high(t + 1)
        before = jnp.where(t == 0, -1, before)
        after = jnp.where(t == trips - 1, now, after)
        for n in (1, 2):
            @pl.when(now + n <= after)
            def _():
                w_start(now + n)
        for n in (1, 0):
            @pl.when(now - n > before)
            def _():
                w_wait(now - n)

        @pl.when(t == (n_tiles - 1) // 2)
        def _():
            for f in (0, 1):
                t_waits[(1, f)].wait_recv()
                x_wait(1, f)
            for copy in (far, to_other[0], to_other[1]):
                copy.start()

        @pl.when(t == (n_tiles - 1) // 2 + 1)
        def _():
            for f in (0, 1):
                t_waits[(2, f)].wait_recv()
                x_wait(2, f)

        @pl.when(t == n_tiles)
        def _():
            x_wait(3, 0)
            to_other[2].start()

        @pl.when(t == 3 * n_tiles // 2)
        def _():
            for f in (0, 1):
                t_waits[(3, f)].wait_recv()
            x_wait(3, 1)

        halves = [place(2 * t), place(2 * t + 1)]
        bias = [jnp.where(j == n_tiles - 1, LOWEST, 0.0).astype(jnp.float32) for j, _, _ in halves]
        for i in range(0, 2 * half_units, 2):
            for n in (i, i + 1):
                e, (s, b) = n // half_units, divmod(n % half_units, blocks)
                _, g, q = halves[e]
                z = lax.dot_general(
                    w_buf[lax.rem(q, W_SLOTS), pl.ds(s * UNIT_ROWS, UNIT_ROWS), :],
                    x_all[g, pl.ds(b * SIDE, SIDE), :],
                    (((1,), (1,)), ((), ())), preferred_element_type=jnp.float32)
                z_buf[n % 4] = z
                z_top[n % 4] = jnp.max(z[overlap if s == 0 else 0:].reshape(-1, 8, SIDE), axis=0)
            for n in (i - 2, i - 1):
                if n < 0:
                    drain_last(jnp.maximum(t - 1, 0), half_units + n, t > 0)
                else:
                    e, (s, b) = n // half_units, divmod(n % half_units, blocks)
                    j, g, _ = halves[e]
                    drain(n % 4, g * blocks + b, me * vocab + row_start(j) + s * UNIT_ROWS,
                          bias[e] if s == 0 else None, tgt_all[g, :, b * SIDE:(b + 1) * SIDE])
        return carry

    lax.fori_loop(0, trips, trip, 0)
    for n in (half_units - 2, half_units - 1):
        drain_last(trips - 1, n, None)

    c1 = c_buf[0:1, :]
    for g in range(chips):
        for b in range(blocks):
            n, lanes = g * blocks + b, slice(b * SIDE, (b + 1) * SIDE)
            m = st_m[n]
            top = jnp.max(m, axis=0, keepdims=True)
            f = jnp.exp2((m - top) * c1)
            stage[g, 0:1, lanes] = top
            stage[g, 1:2, lanes] = jnp.sum(st_s[n] * f, axis=0, keepdims=True)
            stage[g, 2:3, lanes] = jnp.sum(st_w[n] * f, axis=0, keepdims=True)
            stage[g, 3:4, lanes] = jnp.sum(st_t[n], axis=0, keepdims=True)
            stage[g, 4:8, lanes] = jnp.zeros((4, SIDE), jnp.float32)

    def s_copy(where):
        (p, f), (dp, df) = where, SEEN_AS[where]
        return pltpu.make_async_remote_copy(
            src_ref=stage.at[p, :, pl.ds(f * tok, tok)],
            dst_ref=inbox.at[dp * 2 + df],
            send_sem=s_send.at[p * 2 + f],
            recv_sem=s_recv.at[dp * 2 + df],
            device_id=device(*OWNER[where]),
            device_id_type=MESH,
        )

    s_copies = [s_copy(where) for where in OWNER]
    for copy in s_copies:
        copy.start()
    inbox[0] = stage[0, :, 0:tok]
    for copy in s_copies:
        copy.wait()
    got = [inbox[n] for n in range(n_tp)]
    top = functools.reduce(jnp.maximum, [x[0:1] for x in got])
    c2 = jnp.concatenate([c1, c1], axis=1)[:, :tok]
    scales = [jnp.exp2((x[0:1] - top) * c2) for x in got]
    out_ref[0:1, :] = top
    out_ref[1:2, :] = functools.reduce(jnp.add, [x[1:2] * f for x, f in zip(got, scales)])
    out_ref[2:3, :] = functools.reduce(jnp.add, [x[2:3] * f for x, f in zip(got, scales)])
    out_ref[3:4, :] = functools.reduce(jnp.add, [x[3:4] for x in got])

    for copy in own_copies + [far] + to_other + list(t_copies.values()):
        copy.wait_send()


def solution(mesh):
    n_tp = mesh.shape['tp']

    def device_body(h_loc, target_loc, norm_gain, w_loc, tau):
        _, tok, depth = h_loc.shape
        vocab = w_loc.shape[0]
        pair, chips = 2 * tok, n_tp // 2
        blocks = pair // SIDE
        any_space = pl.BlockSpec(memory_space=pl.ANY)
        vmem = pl.BlockSpec(memory_space=pltpu.VMEM)
        stat = pltpu.VMEM((chips * blocks + 1, 8, SIDE), jnp.float32)
        dma = pltpu.SemaphoreType.DMA
        out = pl.pallas_call(
            functools.partial(_kernel, (n_tp, tok, depth, vocab)),
            out_shape=jax.ShapeDtypeStruct((4, tok), jnp.float32),
            in_specs=[any_space, vmem, vmem, pl.BlockSpec(memory_space=pltpu.SMEM), any_space],
            out_specs=vmem,
            scratch_shapes=[
                pltpu.VMEM((tok, depth), jnp.bfloat16),
                pltpu.VMEM((chips, pair, depth), jnp.bfloat16),
                pltpu.VMEM((chips, 1, pair), jnp.int32),
                pltpu.VMEM((W_SLOTS, SUBS * UNIT_ROWS, depth), jnp.bfloat16),
                pltpu.VMEM((4, UNIT_ROWS, SIDE), jnp.float32),
                pltpu.VMEM((4, 8, SIDE), jnp.float32),
                stat, stat, stat, stat,
                pltpu.VMEM((8, SIDE), jnp.float32),
                pltpu.VMEM((chips, 8, pair), jnp.float32),
                pltpu.VMEM((n_tp, 8, tok), jnp.float32),
                dma(()), dma((W_SLOTS, SUBS)), dma((7,)), dma((n_tp,)), dma((n_tp,)), dma((n_tp,)), dma((n_tp,)),
                dma((n_tp,)),
            ],
            compiler_params=pltpu.CompilerParams(
                collective_id=0, has_side_effects=True, vmem_limit_bytes=60 * 1024 * 1024),
        )(h_loc[0], target_loc, norm_gain, tau.reshape(1, 1), w_loc)
        top, total, weighted, target = (out[n:n + 1] for n in range(4))
        log_norm = top / tau + jnp.log(total)
        return target / tau - log_norm, log_norm - (weighted / total) / tau

    return jax.shard_map(
        device_body,
        mesh=mesh,
        in_specs=(P('dp', 'tp', None), P('dp', 'tp'), P(), P('tp', None), P()),
        out_specs=(P('dp', 'tp'), P('dp', 'tp')),
        check_vma=False,
    )
```

```python
import functools

import jax
import jax.numpy as jnp
from jax import lax
from jax.experimental import pallas as pl
from jax.experimental.pallas import tpu as pltpu
from jax.sharding import PartitionSpec as P

NORM_EPS = 1e-6
LOG2E = 1.4426950408889634
LOWEST = -3.4028234e38
SIDE = 256
UNIT_ROWS = 864
SUBS = 2
PIECE = 48
NORM_ROWS = 64
HALVES = 4
W_SLOTS = 2 * HALVES
PIECES = 3
MESH = pl.DeviceIdType.MESH

OWNER = {(0, 1): (0, 1), (1, 0): (-1, 0), (1, 1): (1, 0), (2, 0): (-1, 1), (2, 1): (1, 1), (3, 0): (2, 0), (3, 1): (2, 1)}
SEEN_AS = {(0, 1): (0, 1), (1, 0): (1, 1), (1, 1): (1, 0), (2, 0): (2, 1), (2, 1): (2, 0), (3, 0): (3, 0), (3, 1): (3, 1)}


def _kernel(dims, h_ref, tgt_ref, gain_ref, tau_ref, w_ref, out_ref,
            h_buf, x_all, tgt_all, w_buf, z_buf, z_top, st_m, st_s, st_w, st_t, c_buf, stage, inbox,
            h_sem, w_sem, p_send, p_recv, x_send, x_recv, t_send, t_recv, s_send, s_recv):
    n_tp, tok, depth, vocab = dims
    chips = n_tp // 2
    pair = 2 * tok
    blocks = pair // SIDE
    tile_rows = SUBS * UNIT_ROWS
    n_tiles = -(-vocab // tile_rows)
    overlap = n_tiles * tile_rows - vocab
    half_units = SUBS * blocks
    n_stats = chips * blocks
    me = lax.axis_index('tp')
    x_pos, core = lax.div(me, 2), lax.rem(me, 2)

    def device(hops, other):
        return {'tp': lax.rem(x_pos + hops + chips, chips) * 2 + (1 - core if other else core)}

    def row_start(j):
        return pl.multiple_of(jnp.minimum(j * tile_rows, vocab - tile_rows), 16)

    def w_copy(q, s):
        slot = lax.rem(q, W_SLOTS)
        return pltpu.make_async_copy(
            w_ref.at[pl.ds(pl.multiple_of(row_start(lax.rem(q, n_tiles)) + s * UNIT_ROWS, 16), UNIT_ROWS)],
            w_buf.at[slot, pl.ds(s * UNIT_ROWS, UNIT_ROWS)],
            w_sem.at[slot, s],
        )

    def w_start(q):
        for s in range(SUBS):
            w_copy(q, s).start()

    def w_wait(q):
        for s in range(SUBS):
            w_copy(q, s).wait()

    h_copy = pltpu.make_async_copy(h_ref, h_buf, h_sem)
    h_copy.start()
    for n in range(HALVES):
        w_start(n)
    barrier = pltpu.get_barrier_semaphore()
    for hops, other in OWNER.values():
        pl.semaphore_signal(barrier, inc=1, device_id=device(hops, other), device_id_type=MESH)

    c_buf[...] = LOG2E / jnp.full(c_buf.shape, tau_ref[0, 0], jnp.float32)
    st_m[...] = jnp.full(st_m.shape, LOWEST, jnp.float32)
    for st in (st_s, st_w, st_t):
        st[...] = jnp.zeros(st.shape, jnp.float32)
    z_top[...] = jnp.zeros(z_top.shape, jnp.float32)
    for n in (2, 3):
        z_buf[n] = jnp.zeros(z_buf.shape[1:], jnp.float32)

    h_copy.wait()
    gain = gain_ref[...].astype(jnp.float32).reshape(1, depth)

    piece = tok // PIECES

    def p_copy(n):
        return pltpu.make_async_remote_copy(
            src_ref=x_all.at[0, pl.ds(n * piece, piece)],
            dst_ref=x_all.at[0, pl.ds(tok + n * piece, piece)],
            send_sem=p_send.at[n],
            recv_sem=p_recv.at[n],
            device_id=device(0, 1),
            device_id_type=MESH,
        )

    pl.semaphore_wait(barrier, len(OWNER))
    for n in range(PIECES):
        @pl.loop(0, piece // NORM_ROWS)
        def _(r):
            rows = pl.ds(pl.multiple_of(n * piece + r * NORM_ROWS, 16), NORM_ROWS)
            h = h_buf[rows, :].astype(jnp.float32)
            inv = lax.rsqrt(jnp.mean(h * h, axis=-1, keepdims=True) + NORM_EPS)
            x_all[0, rows, :] = (gain * h * inv).astype(jnp.bfloat16)

        p_copy(n).start()

    def chunk(p, f):
        return x_all.at[p, pl.ds(f * tok if isinstance(f, int) else pl.multiple_of(f * tok, 16), tok)]

    def x_copy(src, dst, hops, other, send):
        return pltpu.make_async_remote_copy(
            src_ref=chunk(*src),
            dst_ref=chunk(*dst),
            send_sem=x_send.at[send],
            recv_sem=x_recv.at[dst[0] * 2 + dst[1]],
            device_id=device(hops, other),
            device_id_type=MESH,
        )

    def x_wait(p, f):
        x_copy((p, f), (p, f), 0, 1, 0).wait_recv()

    def t_copy(where):
        p, f = SEEN_AS[where]
        return pltpu.make_async_remote_copy(
            src_ref=tgt_ref,
            dst_ref=tgt_all.at[p, :, pl.ds(f * tok, tok)],
            send_sem=t_send.at[where[0] * 2 + where[1]],
            recv_sem=t_recv.at[p * 2 + f],
            device_id=device(*OWNER[where]),
            device_id_type=MESH,
        )

    t_copies = {where: t_copy(where) for where in OWNER}
    t_waits = {SEEN_AS[where]: copy for where, copy in t_copies.items()}
    for copy in t_copies.values():
        copy.start()
    own_copies = [x_copy((0, 0), (1, 0), 1, 0, 1), x_copy((0, 0), (1, 1), -1, 0, 2)]
    for copy in own_copies:
        copy.start()
    tgt_all[0, :, 0:tok] = tgt_ref[...]

    far = x_copy((1, jnp.where(core == 0, 0, 1)), (3, 0), jnp.where(core == 0, 1, -1), 0, 3)
    to_other = [x_copy((1, 0), (2, 0), 0, 1, 4), x_copy((1, 1), (2, 1), 0, 1, 5), x_copy((3, 0), (3, 1), 0, 1, 6)]

    t_waits[(0, 1)].wait_recv()
    for n in range(PIECES):
        p_copy(n).wait_recv()

    sublane = lax.broadcasted_iota(jnp.int32, (8, SIDE), 0)

    def place(h):
        late = h >= 3 * n_tiles
        first = h < n_tiles
        u = jnp.maximum(h - n_tiles, 0)
        j = jnp.where(first, h, jnp.where(late, h - 3 * n_tiles, lax.div(u, 2)))
        g = jnp.where(first, 0, jnp.where(late, 3, 1 + lax.rem(u, 2)))
        q = jnp.where(first, h, jnp.where(late, h - n_tiles, n_tiles + lax.div(u, 2)))
        return j, g, q

    def drain(slot, stat, base, bias, target):
        m_old = st_m[stat]
        top = jnp.maximum(m_old, z_top[slot])
        if bias is not None:
            head = z_buf[slot, 0:overlap, :].reshape(overlap // 8, 8, SIDE) + bias
            top = jnp.maximum(top, jnp.max(head, axis=0))
        c = c_buf[...]
        alpha = jnp.exp2((m_old - top) * c)
        st_m[stat] = top
        total, weighted, hit = st_s[stat] * alpha, st_w[stat] * alpha, st_t[stat]
        row = target - sublane - base
        for r in range(0, UNIT_ROWS, PIECE):
            z = z_buf[slot, pl.ds(r, PIECE), :].reshape(PIECE // 8, 8, SIDE)
            zb = z
            if bias is not None and r == 0:
                zb = jnp.concatenate([z[:overlap // 8] + bias, z[overlap // 8:]], axis=0)
            p = jnp.exp2((zb - top) * c)
            total = total + jnp.sum(p, axis=0)
            weighted = weighted + jnp.sum(p * z, axis=0)
            for i in range(PIECE // 8):
                hit = jnp.where(row == r + 8 * i, z[i], hit)
        st_s[stat], st_w[stat], st_t[stat] = total, weighted, hit

    def high(t):
        return place(HALVES * t + HALVES - 1)[2]

    trips = n_tiles * chips // HALVES

    def drain_last(t, i, valid):
        j, g, _ = place(HALVES * t + HALVES - 1)
        s, b = divmod(i, blocks)
        stat = g * blocks + b if valid is None else jnp.where(valid, g * blocks + b, n_stats)
        drain(2 + (i - (half_units - 2)), stat, me * vocab + row_start(j) + s * UNIT_ROWS, None,
              tgt_all[g, :, b * SIDE:(b + 1) * SIDE])

    def trip(t, carry):
        now, before, after = high(t), high(t - 1), high(t + 1)
        before = jnp.where(t == 0, -1, before)
        after = jnp.where(t == trips - 1, now, after)
        for n in range(1, HALVES + 1):
            @pl.when(now + n <= after)
            def _():
                w_start(now + n)
        for n in range(HALVES - 1, -1, -1):
            @pl.when(now - n > before)
            def _():
                w_wait(now - n)

        @pl.when(t == n_tiles // HALVES)
        def _():
            for f in (0, 1):
                t_waits[(1, f)].wait_recv()
                x_wait(1, f)
            for copy in (far, to_other[0], to_other[1]):
                copy.start()

        @pl.when(t == (n_tiles + 1) // HALVES)
        def _():
            for f in (0, 1):
                t_waits[(2, f)].wait_recv()
                x_wait(2, f)

        @pl.when(t == 2 * n_tiles // HALVES)
        def _():
            x_wait(3, 0)
            to_other[2].start()

        @pl.when(t == 3 * n_tiles // HALVES)
        def _():
            for f in (0, 1):
                t_waits[(3, f)].wait_recv()
            x_wait(3, 1)

        halves = [place(HALVES * t + e) for e in range(HALVES)]
        bias = [jnp.where(j == n_tiles - 1, LOWEST, 0.0).astype(jnp.float32) for j, _, _ in halves]
        for i in range(0, HALVES * half_units, 2):
            for n in (i, i + 1):
                e, (s, b) = n // half_units, divmod(n % half_units, blocks)
                _, g, q = halves[e]
                z = lax.dot_general(
                    w_buf[lax.rem(q, W_SLOTS), pl.ds(s * UNIT_ROWS, UNIT_ROWS), :],
                    x_all[g, pl.ds(b * SIDE, SIDE), :],
                    (((1,), (1,)), ((), ())), preferred_element_type=jnp.float32)
                z_buf[n % 4] = z
                z_top[n % 4] = jnp.max(z[overlap if s == 0 else 0:].reshape(-1, 8, SIDE), axis=0)
            for n in (i - 2, i - 1):
                if n < 0:
                    drain_last(jnp.maximum(t - 1, 0), half_units + n, t > 0)
                else:
                    e, (s, b) = n // half_units, divmod(n % half_units, blocks)
                    j, g, _ = halves[e]
                    drain(n % 4, g * blocks + b, me * vocab + row_start(j) + s * UNIT_ROWS,
                          bias[e] if s == 0 else None, tgt_all[g, :, b * SIDE:(b + 1) * SIDE])
        return carry

    lax.fori_loop(0, trips, trip, 0)
    for n in (half_units - 2, half_units - 1):
        drain_last(trips - 1, n, None)

    c1 = c_buf[0:1, :]
    for g in range(chips):
        for b in range(blocks):
            n, lanes = g * blocks + b, slice(b * SIDE, (b + 1) * SIDE)
            m = st_m[n]
            top = jnp.max(m, axis=0, keepdims=True)
            f = jnp.exp2((m - top) * c1)
            stage[g, 0:1, lanes] = top
            stage[g, 1:2, lanes] = jnp.sum(st_s[n] * f, axis=0, keepdims=True)
            stage[g, 2:3, lanes] = jnp.sum(st_w[n] * f, axis=0, keepdims=True)
            stage[g, 3:4, lanes] = jnp.sum(st_t[n], axis=0, keepdims=True)
            stage[g, 4:8, lanes] = jnp.zeros((4, SIDE), jnp.float32)

    def s_copy(where):
        (p, f), (dp, df) = where, SEEN_AS[where]
        return pltpu.make_async_remote_copy(
            src_ref=stage.at[p, :, pl.ds(f * tok, tok)],
            dst_ref=inbox.at[dp * 2 + df],
            send_sem=s_send.at[p * 2 + f],
            recv_sem=s_recv.at[dp * 2 + df],
            device_id=device(*OWNER[where]),
            device_id_type=MESH,
        )

    s_copies = [s_copy(where) for where in OWNER]
    for copy in s_copies:
        copy.start()
    inbox[0] = stage[0, :, 0:tok]
    for copy in s_copies:
        copy.wait()
    got = [inbox[n] for n in range(n_tp)]
    top = functools.reduce(jnp.maximum, [x[0:1] for x in got])
    c2 = jnp.concatenate([c1, c1], axis=1)[:, :tok]
    scales = [jnp.exp2((x[0:1] - top) * c2) for x in got]
    out_ref[0:1, :] = top
    out_ref[1:2, :] = functools.reduce(jnp.add, [x[1:2] * f for x, f in zip(got, scales)])
    out_ref[2:3, :] = functools.reduce(jnp.add, [x[2:3] * f for x, f in zip(got, scales)])
    out_ref[3:4, :] = functools.reduce(jnp.add, [x[3:4] for x in got])

    for copy in [p_copy(n) for n in range(PIECES)] + own_copies + [far] + to_other + list(t_copies.values()):
        copy.wait_send()


def _finish(tau_ref, stats_ref, lp_ref, ent_ref):
    top, total, weighted, target = (stats_ref[n:n + 1, :] for n in range(4))
    tau = jnp.full(top.shape, tau_ref[0, 0], jnp.float32)
    log_norm = top / tau + jnp.log(total)
    lp_ref[...] = target / tau - log_norm
    ent_ref[...] = log_norm - (weighted / total) / tau


def solution(mesh):
    n_tp = mesh.shape['tp']

    def device_body(h_loc, target_loc, norm_gain, w_loc, tau):
        _, tok, depth = h_loc.shape
        vocab = w_loc.shape[0]
        pair, chips = 2 * tok, n_tp // 2
        blocks = pair // SIDE
        any_space = pl.BlockSpec(memory_space=pl.ANY)
        vmem = pl.BlockSpec(memory_space=pltpu.VMEM)
        stat = pltpu.VMEM((chips * blocks + 1, 8, SIDE), jnp.float32)
        dma = pltpu.SemaphoreType.DMA
        out = pl.pallas_call(
            functools.partial(_kernel, (n_tp, tok, depth, vocab)),
            out_shape=jax.ShapeDtypeStruct((4, tok), jnp.float32),
            in_specs=[any_space, vmem, vmem, pl.BlockSpec(memory_space=pltpu.SMEM), any_space],
            out_specs=vmem,
            scratch_shapes=[
                pltpu.VMEM((tok, depth), jnp.bfloat16),
                pltpu.VMEM((chips, pair, depth), jnp.bfloat16),
                pltpu.VMEM((chips, 1, pair), jnp.int32),
                pltpu.VMEM((W_SLOTS, SUBS * UNIT_ROWS, depth), jnp.bfloat16),
                pltpu.VMEM((4, UNIT_ROWS, SIDE), jnp.float32),
                pltpu.VMEM((4, 8, SIDE), jnp.float32),
                stat, stat, stat, stat,
                pltpu.VMEM((8, SIDE), jnp.float32),
                pltpu.VMEM((chips, 8, pair), jnp.float32),
                pltpu.VMEM((n_tp, 8, tok), jnp.float32),
                dma(()), dma((W_SLOTS, SUBS)), dma((PIECES,)), dma((PIECES,)), dma((7,)), dma((n_tp,)), dma((n_tp,)), dma((n_tp,)), dma((n_tp,)),
                dma((n_tp,)),
            ],
            compiler_params=pltpu.CompilerParams(
                collective_id=0, has_side_effects=True, vmem_limit_bytes=62 * 1024 * 1024),
        )(h_loc[0], target_loc, norm_gain, tau.reshape(1, 1), w_loc)
        row = jax.ShapeDtypeStruct((1, tok), jnp.float32)
        return pl.pallas_call(
            _finish,
            out_shape=(row, row),
            in_specs=[pl.BlockSpec(memory_space=pltpu.SMEM), vmem],
            out_specs=(vmem, vmem),
        )(tau.reshape(1, 1), out)

    return jax.shard_map(
        device_body,
        mesh=mesh,
        in_specs=(P('dp', 'tp', None), P('dp', 'tp'), P(), P('tp', None), P()),
        out_specs=(P('dp', 'tp'), P('dp', 'tp')),
        check_vma=False,
    )
```

```python
import functools

import jax
import jax.numpy as jnp
from jax import lax
from jax.experimental import pallas as pl
from jax.experimental.pallas import tpu as pltpu
from jax.sharding import PartitionSpec as P

NORM_EPS = 1e-6
LOG2E = 1.4426950408889634
LOWEST = -3.4028234e38
SIDE = 256
UNIT_ROWS = 864
SUBS = 2
PIECE = 48
NORM_ROWS = 64
HALVES = 2
W_SLOTS = 2 * HALVES
PIECES = 3
MESH = pl.DeviceIdType.MESH

OWNER = {(0, 1): (0, 1), (1, 0): (-1, 0), (1, 1): (1, 0), (2, 0): (-1, 1), (2, 1): (1, 1), (3, 0): (2, 0), (3, 1): (2, 1)}
SEEN_AS = {(0, 1): (0, 1), (1, 0): (1, 1), (1, 1): (1, 0), (2, 0): (2, 1), (2, 1): (2, 0), (3, 0): (3, 0), (3, 1): (3, 1)}


def _kernel(dims, h_ref, tgt_ref, gain_ref, tau_ref, w_ref, out_ref,
            h_buf, x_all, tgt_all, w_buf, z_buf, z_top, st_m, st_s, st_w, st_t, c_buf, stage, inbox,
            h_sem, w_sem, p_send, p_recv, x_send, x_recv, t_send, t_recv, s_send, s_recv):
    n_tp, tok, depth, vocab = dims
    chips = n_tp // 2
    pair = 2 * tok
    blocks = pair // SIDE
    tile_rows = SUBS * UNIT_ROWS
    n_tiles = -(-vocab // tile_rows)
    overlap = n_tiles * tile_rows - vocab
    half_units = SUBS * blocks
    n_stats = chips * blocks
    me = lax.axis_index('tp')
    x_pos, core = lax.div(me, 2), lax.rem(me, 2)

    def device(hops, other):
        return {'tp': lax.rem(x_pos + hops + chips, chips) * 2 + (1 - core if other else core)}

    def row_start(j):
        return pl.multiple_of(jnp.minimum(j * tile_rows, vocab - tile_rows), 16)

    def w_copy(q, s):
        slot = lax.rem(q, W_SLOTS)
        return pltpu.make_async_copy(
            w_ref.at[pl.ds(pl.multiple_of(row_start(lax.rem(q, n_tiles)) + s * UNIT_ROWS, 16), UNIT_ROWS)],
            w_buf.at[slot, pl.ds(s * UNIT_ROWS, UNIT_ROWS)],
            w_sem.at[slot, s],
        )

    def w_start(q):
        for s in range(SUBS):
            w_copy(q, s).start()

    def w_wait(q):
        for s in range(SUBS):
            w_copy(q, s).wait()

    h_copy = pltpu.make_async_copy(h_ref, h_buf, h_sem)
    h_copy.start()
    for n in range(HALVES):
        w_start(n)
    barrier = pltpu.get_barrier_semaphore()
    for hops, other in OWNER.values():
        pl.semaphore_signal(barrier, inc=1, device_id=device(hops, other), device_id_type=MESH)

    c_buf[...] = LOG2E / jnp.full(c_buf.shape, tau_ref[0, 0], jnp.float32)
    st_m[...] = jnp.full(st_m.shape, LOWEST, jnp.float32)
    for st in (st_s, st_w, st_t):
        st[...] = jnp.zeros(st.shape, jnp.float32)
    z_top[...] = jnp.zeros(z_top.shape, jnp.float32)
    for n in (2, 3):
        z_buf[n] = jnp.zeros(z_buf.shape[1:], jnp.float32)

    h_copy.wait()
    gain = gain_ref[...].astype(jnp.float32).reshape(1, depth)

    piece = tok // PIECES

    def p_copy(n):
        return pltpu.make_async_remote_copy(
            src_ref=x_all.at[0, pl.ds(n * piece, piece)],
            dst_ref=x_all.at[0, pl.ds(tok + n * piece, piece)],
            send_sem=p_send.at[n],
            recv_sem=p_recv.at[n],
            device_id=device(0, 1),
            device_id_type=MESH,
        )

    pl.semaphore_wait(barrier, len(OWNER))
    for n in range(PIECES):
        @pl.loop(0, piece // NORM_ROWS)
        def _(r):
            rows = pl.ds(pl.multiple_of(n * piece + r * NORM_ROWS, 16), NORM_ROWS)
            h = h_buf[rows, :].astype(jnp.float32)
            inv = lax.rsqrt(jnp.mean(h * h, axis=-1, keepdims=True) + NORM_EPS)
            x_all[0, rows, :] = (gain * h * inv).astype(jnp.bfloat16)

        p_copy(n).start()

    def chunk(p, f):
        return x_all.at[p, pl.ds(f * tok if isinstance(f, int) else pl.multiple_of(f * tok, 16), tok)]

    def x_copy(src, dst, hops, other, send):
        return pltpu.make_async_remote_copy(
            src_ref=chunk(*src),
            dst_ref=chunk(*dst),
            send_sem=x_send.at[send],
            recv_sem=x_recv.at[dst[0] * 2 + dst[1]],
            device_id=device(hops, other),
            device_id_type=MESH,
        )

    def x_wait(p, f):
        x_copy((p, f), (p, f), 0, 1, 0).wait_recv()

    def t_copy(where):
        p, f = SEEN_AS[where]
        return pltpu.make_async_remote_copy(
            src_ref=tgt_ref,
            dst_ref=tgt_all.at[p, :, pl.ds(f * tok, tok)],
            send_sem=t_send.at[where[0] * 2 + where[1]],
            recv_sem=t_recv.at[p * 2 + f],
            device_id=device(*OWNER[where]),
            device_id_type=MESH,
        )

    t_copies = {where: t_copy(where) for where in OWNER}
    t_waits = {SEEN_AS[where]: copy for where, copy in t_copies.items()}
    t_copies[(0, 1)].start()
    own_copies = [x_copy((0, 0), (1, 0), 1, 0, 1), x_copy((0, 0), (1, 1), -1, 0, 2)]
    tgt_all[0, :, 0:tok] = tgt_ref[...]

    far = x_copy((1, jnp.where(core == 0, 0, 1)), (3, 0), jnp.where(core == 0, 1, -1), 0, 3)
    to_other = [x_copy((1, 0), (2, 0), 0, 1, 4), x_copy((1, 1), (2, 1), 0, 1, 5), x_copy((3, 0), (3, 1), 0, 1, 6)]

    t_waits[(0, 1)].wait_recv()
    for n in range(PIECES):
        p_copy(n).wait_recv()
    for where, copy in t_copies.items():
        if where != (0, 1):
            copy.start()
    for copy in own_copies:
        copy.start()

    sublane = lax.broadcasted_iota(jnp.int32, (8, SIDE), 0)

    def place(h):
        late = h >= 3 * n_tiles
        first = h < n_tiles
        u = jnp.maximum(h - n_tiles, 0)
        j = jnp.where(first, h, jnp.where(late, h - 3 * n_tiles, lax.div(u, 2)))
        g = jnp.where(first, 0, jnp.where(late, 3, 1 + lax.rem(u, 2)))
        q = jnp.where(first, h, jnp.where(late, h - n_tiles, n_tiles + lax.div(u, 2)))
        return j, g, q

    def drain(slot, stat, base, bias, target):
        m_old = st_m[stat]
        top = jnp.maximum(m_old, z_top[slot])
        if bias is not None:
            head = z_buf[slot, 0:overlap, :].reshape(overlap // 8, 8, SIDE) + bias
            top = jnp.maximum(top, jnp.max(head, axis=0))
        c = c_buf[...]
        alpha = jnp.exp2((m_old - top) * c)
        st_m[stat] = top
        total, weighted, hit = st_s[stat] * alpha, st_w[stat] * alpha, st_t[stat]
        row = target - sublane - base
        for r in range(0, UNIT_ROWS, PIECE):
            z = z_buf[slot, pl.ds(r, PIECE), :].reshape(PIECE // 8, 8, SIDE)
            zb = z
            if bias is not None and r == 0:
                zb = jnp.concatenate([z[:overlap // 8] + bias, z[overlap // 8:]], axis=0)
            p = jnp.exp2((zb - top) * c)
            total = total + jnp.sum(p, axis=0)
            weighted = weighted + jnp.sum(p * z, axis=0)
            for i in range(PIECE // 8):
                hit = jnp.where(row == r + 8 * i, z[i], hit)
        st_s[stat], st_w[stat], st_t[stat] = total, weighted, hit

    def high(t):
        return place(HALVES * t + HALVES - 1)[2]

    trips = n_tiles * chips // HALVES

    def drain_last(t, i, valid):
        j, g, _ = place(HALVES * t + HALVES - 1)
        s, b = divmod(i, blocks)
        stat = g * blocks + b if valid is None else jnp.where(valid, g * blocks + b, n_stats)
        drain(2 + (i - (half_units - 2)), stat, me * vocab + row_start(j) + s * UNIT_ROWS, None,
              tgt_all[g, :, b * SIDE:(b + 1) * SIDE])

    def trip(t, carry):
        now, before, after = high(t), high(t - 1), high(t + 1)
        before = jnp.where(t == 0, -1, before)
        after = jnp.where(t == trips - 1, now, after)
        for n in range(1, HALVES + 1):
            @pl.when(now + n <= after)
            def _():
                w_start(now + n)
        for n in range(HALVES - 1, -1, -1):
            @pl.when(now - n > before)
            def _():
                w_wait(now - n)

        @pl.when(t == n_tiles // HALVES - 1)
        def _():
            for f in (0, 1):
                t_waits[(1, f)].wait_recv()
                x_wait(1, f)
            for copy in (far, to_other[0], to_other[1]):
                copy.start()

        @pl.when(t == (n_tiles + 1) // HALVES)
        def _():
            for f in (0, 1):
                t_waits[(2, f)].wait_recv()
                x_wait(2, f)

        @pl.when(t == 2 * n_tiles // HALVES)
        def _():
            x_wait(3, 0)
            to_other[2].start()

        @pl.when(t == 3 * n_tiles // HALVES)
        def _():
            for f in (0, 1):
                t_waits[(3, f)].wait_recv()
            x_wait(3, 1)

        halves = [place(HALVES * t + e) for e in range(HALVES)]
        bias = [jnp.where(j == n_tiles - 1, LOWEST, 0.0).astype(jnp.float32) for j, _, _ in halves]
        for i in range(0, HALVES * half_units, 2):
            for n in (i, i + 1):
                e, (s, b) = n // half_units, divmod(n % half_units, blocks)
                _, g, q = halves[e]
                z = lax.dot_general(
                    w_buf[lax.rem(q, W_SLOTS), pl.ds(s * UNIT_ROWS, UNIT_ROWS), :],
                    x_all[g, pl.ds(b * SIDE, SIDE), :],
                    (((1,), (1,)), ((), ())), preferred_element_type=jnp.float32)
                z_buf[n % 4] = z
                z_top[n % 4] = jnp.max(z[overlap if s == 0 else 0:].reshape(-1, 8, SIDE), axis=0)
            for n in (i - 2, i - 1):
                if n < 0:
                    drain_last(jnp.maximum(t - 1, 0), half_units + n, t > 0)
                else:
                    e, (s, b) = n // half_units, divmod(n % half_units, blocks)
                    j, g, _ = halves[e]
                    drain(n % 4, g * blocks + b, me * vocab + row_start(j) + s * UNIT_ROWS,
                          bias[e] if s == 0 else None, tgt_all[g, :, b * SIDE:(b + 1) * SIDE])
        return carry

    lax.fori_loop(0, trips, trip, 0)
    for n in (half_units - 2, half_units - 1):
        drain_last(trips - 1, n, None)

    c1 = c_buf[0:1, :]
    for g in range(chips):
        for b in range(blocks):
            n, lanes = g * blocks + b, slice(b * SIDE, (b + 1) * SIDE)
            m = st_m[n]
            top = jnp.max(m, axis=0, keepdims=True)
            f = jnp.exp2((m - top) * c1)
            stage[g, 0:1, lanes] = top
            stage[g, 1:2, lanes] = jnp.sum(st_s[n] * f, axis=0, keepdims=True)
            stage[g, 2:3, lanes] = jnp.sum(st_w[n] * f, axis=0, keepdims=True)
            stage[g, 3:4, lanes] = jnp.sum(st_t[n], axis=0, keepdims=True)
            stage[g, 4:8, lanes] = jnp.zeros((4, SIDE), jnp.float32)

    def s_copy(where):
        (p, f), (dp, df) = where, SEEN_AS[where]
        return pltpu.make_async_remote_copy(
            src_ref=stage.at[p, :, pl.ds(f * tok, tok)],
            dst_ref=inbox.at[dp * 2 + df],
            send_sem=s_send.at[p * 2 + f],
            recv_sem=s_recv.at[dp * 2 + df],
            device_id=device(*OWNER[where]),
            device_id_type=MESH,
        )

    s_copies = [s_copy(where) for where in OWNER]
    for copy in s_copies:
        copy.start()
    inbox[0] = stage[0, :, 0:tok]
    for copy in s_copies:
        copy.wait()
    got = [inbox[n] for n in range(n_tp)]
    top = functools.reduce(jnp.maximum, [x[0:1] for x in got])
    c2 = jnp.concatenate([c1, c1], axis=1)[:, :tok]
    scales = [jnp.exp2((x[0:1] - top) * c2) for x in got]
    out_ref[0:1, :] = top
    out_ref[1:2, :] = functools.reduce(jnp.add, [x[1:2] * f for x, f in zip(got, scales)])
    out_ref[2:3, :] = functools.reduce(jnp.add, [x[2:3] * f for x, f in zip(got, scales)])
    out_ref[3:4, :] = functools.reduce(jnp.add, [x[3:4] for x in got])

    for copy in [p_copy(n) for n in range(PIECES)] + own_copies + [far] + to_other + list(t_copies.values()):
        copy.wait_send()


def _finish(tau_ref, stats_ref, lp_ref, ent_ref):
    top, total, weighted, target = (stats_ref[n:n + 1, :] for n in range(4))
    tau = jnp.full(top.shape, tau_ref[0, 0], jnp.float32)
    log_norm = top / tau + jnp.log(total)
    lp_ref[...] = target / tau - log_norm
    ent_ref[...] = log_norm - (weighted / total) / tau


def solution(mesh):
    n_tp = mesh.shape['tp']

    def device_body(h_loc, target_loc, norm_gain, w_loc, tau):
        _, tok, depth = h_loc.shape
        vocab = w_loc.shape[0]
        pair, chips = 2 * tok, n_tp // 2
        blocks = pair // SIDE
        any_space = pl.BlockSpec(memory_space=pl.ANY)
        vmem = pl.BlockSpec(memory_space=pltpu.VMEM)
        stat = pltpu.VMEM((chips * blocks + 1, 8, SIDE), jnp.float32)
        dma = pltpu.SemaphoreType.DMA
        out = pl.pallas_call(
            functools.partial(_kernel, (n_tp, tok, depth, vocab)),
            out_shape=jax.ShapeDtypeStruct((4, tok), jnp.float32),
            in_specs=[any_space, vmem, vmem, pl.BlockSpec(memory_space=pltpu.SMEM), any_space],
            out_specs=vmem,
            scratch_shapes=[
                pltpu.VMEM((tok, depth), jnp.bfloat16),
                pltpu.VMEM((chips, pair, depth), jnp.bfloat16),
                pltpu.VMEM((chips, 1, pair), jnp.int32),
                pltpu.VMEM((W_SLOTS, SUBS * UNIT_ROWS, depth), jnp.bfloat16),
                pltpu.VMEM((4, UNIT_ROWS, SIDE), jnp.float32),
                pltpu.VMEM((4, 8, SIDE), jnp.float32),
                stat, stat, stat, stat,
                pltpu.VMEM((8, SIDE), jnp.float32),
                pltpu.VMEM((chips, 8, pair), jnp.float32),
                pltpu.VMEM((n_tp, 8, tok), jnp.float32),
                dma(()), dma((W_SLOTS, SUBS)), dma((PIECES,)), dma((PIECES,)), dma((7,)), dma((n_tp,)), dma((n_tp,)), dma((n_tp,)), dma((n_tp,)),
                dma((n_tp,)),
            ],
            compiler_params=pltpu.CompilerParams(
                collective_id=0, has_side_effects=True, vmem_limit_bytes=62 * 1024 * 1024),
        )(h_loc[0], target_loc, norm_gain, tau.reshape(1, 1), w_loc)
        row = jax.ShapeDtypeStruct((1, tok), jnp.float32)
        return pl.pallas_call(
            _finish,
            out_shape=(row, row),
            in_specs=[pl.BlockSpec(memory_space=pltpu.SMEM), vmem],
            out_specs=(vmem, vmem),
        )(tau.reshape(1, 1), out)

    return jax.shard_map(
        device_body,
        mesh=mesh,
        in_specs=(P('dp', 'tp', None), P('dp', 'tp'), P(), P('tp', None), P()),
        out_specs=(P('dp', 'tp'), P('dp', 'tp')),
        check_vma=False,
    )
```
